512 devices in a mesh: kgrp: 128 (over y, x, z_hi), img: 4 (over z_lo, core).
Axes of the slice: x: 4, y: 8, z: 8 (z_hi: 4, z_lo: 2; z = z_hi * 2 + z_lo), core: 2. Of those that a mesh axis runs over, the one named last changes fastest.
Arguments:
- vectors: float32 [2, 16, 16384], P(None, 'img', 'kgrp'), may hold values from -6 to 6
- conduction: bfloat16 [256, 2, 8, 4, 4096], P('kgrp', None, None, 'img'), may hold values from -6 to 6
- valence: bfloat16 [256, 2, 8, 4, 4096], P('kgrp', None, None, 'img'), may hold values from -6 to 6
- hole_point: int32 [1], replicated, may hold values from 0 to 16383
- kpoint_grid: int32 [3, 256], replicated, may hold values from 0 to 11
- image_cells: int32 [3, 512], replicated, may hold values from -6 to 6
Outputs:
- psi_real: float32 [16, 4, 4096, 512], P(None, 'img', 'kgrp')
- psi_imag: float32 [16, 4, 4096, 512], P(None, 'img', 'kgrp')
The draws below stay inside these ranges and needn't reach their ends.
All inputs are finite; a program needn't handle non-finite values.
Results may differ from the reference program's by a relative error of at most 0.0043.
Values may be sent and summed in bfloat16 or wider, within the bound.
A program may use at most 64 MiB of HBM per device.

```python
import jax
import jax.numpy as jnp
import numpy as np
from jax import lax

S = 16
NV = 8
NC = 8
NPTS = 16384
NR = 512
K = 256
NT = 16384
SLABS = 4
SLAB_PTS = 4096
N_KGRP = 128


def set_ends(values, rng, least, largest):
    spot = [jax.random.randint(jax.random.fold_in(rng, axis), (), 0, length) for axis, length in enumerate(values.shape)]
    longest = values.shape.index(max(values.shape))
    beside = spot[:longest] + [(spot[longest] + 1) % values.shape[longest]] + spot[longest + 1:]
    return values.at[tuple(spot)].set(least).at[tuple(beside)].set(largest)


def block_levels(stream_key, shape, split, low, high):
    def one(position, parts):
        draws = jax.random.uniform(jax.random.fold_in(jax.random.fold_in(stream_key, 6), position), (parts,), jnp.float32, low / len(split), high / len(split))
        return jnp.repeat(jnp.exp(draws), shape[position] // parts).reshape((-1,) + (1,) * (len(shape) - position - 1))

    factor_of = one(*split[0])
    for cut in split[1:]:
        factor_of = factor_of * one(*cut)
    return factor_of


def noise(key, shape, width, limit, split=(), held_as=jnp.bfloat16):
    values = width * jax.random.normal(key, shape, jnp.float32)
    if split:
        values = values * block_levels(key, shape, split, -0.22, 0.18)
    return jnp.clip(values, -limit, limit).astype(held_as)


def setup_inputs(seed: int = 0) -> dict:
    arg_keys = jax.random.split(jax.random.key(seed), 7)
    vectors = noise(arg_keys[0], (2, S, NT), 1.0, 6.0, ((1, 4), (2, 128)), jnp.float32)
    conduction = noise(arg_keys[1], (K, 2, NC, SLABS, SLAB_PTS), 1.0, 6.0, ((0, 128), (3, 4)))
    valence = noise(arg_keys[2], (K, 2, NV, SLABS, SLAB_PTS), 1.0, 6.0, ((0, 128), (3, 4)))
    hole_point = jax.random.randint(arg_keys[3], (1,), 0, NPTS).astype(jnp.int32)
    kpoint_grid = set_ends(jax.random.randint(arg_keys[4], (3, K), 0, 12), jax.random.fold_in(arg_keys[4], 1), 0, 11).astype(jnp.int32)
    image_cells = set_ends(jax.random.randint(arg_keys[5], (3, NR), -6, 7), jax.random.fold_in(arg_keys[5], 1), -6, 6).astype(jnp.int32)
    return {"vectors": vectors, "conduction": conduction, "valence": valence, "hole_point": hole_point, "kpoint_grid": kpoint_grid, "image_cells": image_cells}


cosine_levels = np.cos(2.0 * np.pi * np.arange(12) / 12.0)
sine_levels = np.sin(2.0 * np.pi * np.arange(12) / 12.0)


def phase_table(kpoint_grid, image_cells):
    turn_count = kpoint_grid[0][:, None] * image_cells[0][None, :]
    turn_count = turn_count + kpoint_grid[1][:, None] * image_cells[1][None, :]
    turn_count = turn_count + kpoint_grid[2][:, None] * image_cells[2][None, :]
    turn_count = jnp.mod(turn_count, 12)
    cosine = jnp.zeros(turn_count.shape, jnp.float32)
    sine_part = jnp.zeros(turn_count.shape, jnp.float32)
    for level_index in range(12):
        matches = turn_count == level_index
        cosine = jnp.where(matches, jnp.float32(cosine_levels[level_index]), cosine)
        sine_part = jnp.where(matches, jnp.float32(sine_levels[level_index]), sine_part)
    upper_half = jnp.stack([cosine, sine_part], 1)
    lower_half = jnp.stack([-sine_part, cosine], 1)
    return jnp.stack([upper_half, lower_half], 0).astype(jnp.bfloat16)


def hole_weights(amplitudes, hole_values):
    norm_factor = (NV * NC) ** -0.5
    real_amplitude = amplitudes[0]
    imaginary_amplitude = amplitudes[1]
    real_hole = hole_values[:, 0]
    imaginary_hole = hole_values[:, 1]
    highest = lax.Precision.HIGHEST
    weight_real = jnp.einsum("skvc,kv->ksc", real_amplitude, real_hole, precision=highest)
    weight_real = weight_real + jnp.einsum("skvc,kv->ksc", imaginary_amplitude, imaginary_hole, precision=highest)
    weight_imaginary = jnp.einsum("skvc,kv->ksc", imaginary_amplitude, real_hole, precision=highest)
    weight_imaginary = weight_imaginary - jnp.einsum("skvc,kv->ksc", real_amplitude, imaginary_hole, precision=highest)
    return jnp.stack([weight_real * norm_factor, weight_imaginary * norm_factor], 1).astype(jnp.bfloat16)


def mixing(weights):
    weight_real = weights[:, 0]
    weight_imaginary = weights[:, 1]
    first_row = jnp.stack([weight_real, -weight_imaginary], 2)
    second_row = jnp.stack([weight_imaginary, weight_real], 2)
    return jnp.stack([first_row, second_row], 1)


def reference(vectors, conduction, valence, hole_point, kpoint_grid, image_cells):
    group_size = N_KGRP
    blocks = NT // (group_size * group_size)
    ordered = vectors.reshape(2, S, group_size, group_size, blocks)
    ordered = ordered.transpose(0, 1, 3, 2, 4).reshape(2, S, K, NV, NC)
    flat_val = valence.reshape(K, 2, NV, NPTS)
    hole_values = lax.dynamic_slice_in_dim(flat_val, hole_point[0].astype(jnp.int32), 1, 3)[..., 0].astype(jnp.float32)
    weights = hole_weights(ordered, hole_values)
    coupling = mixing(weights).astype(jnp.float32)
    phases = phase_table(kpoint_grid, image_cells).astype(jnp.float32)
    flat_cond = conduction.reshape(K, 2, NC, NPTS)
    block_width = 512
    highest = lax.Precision.HIGHEST

    def one_block(offset):
        cond_block = lax.dynamic_slice_in_dim(flat_cond, offset, block_width, 3).astype(jnp.float32)
        products = jnp.einsum("kasbc,kbcp->sakp", coupling, cond_block, precision=highest).astype(jnp.bfloat16)
        products = lax.optimization_barrier(products).astype(jnp.float32)
        return jnp.einsum("sakp,akbn->spbn", products, phases, precision=highest)

    starts = (jnp.arange(NPTS // block_width) * block_width).astype(jnp.int32)
    summed = lax.map(one_block, starts)
    summed = summed.transpose(1, 0, 2, 3, 4).reshape(S, SLABS, SLAB_PTS, 2, NR) * (2 * K) ** -0.5
    return summed[:, :, :, 0, :], summed[:, :, :, 1, :]
```

```python
import functools

import jax
import jax.numpy as jnp
import numpy as np
from jax import lax
from jax.experimental import pallas as pl
from jax.experimental.pallas import tpu as pltpu
from jax.sharding import PartitionSpec as P

MESH = pl.DeviceIdType.MESH
RING = (8, 4, 4)
NV = 8
NC = 8
LANES = 128
PTS = 32


def drain(sem, ref):
    pltpu.make_async_copy(ref, ref, sem).wait()


def exchange(
    ring,
    groups,
    nc,
    hole_ref,
    vec_ref,
    cond_hbm,
    val_hbm,
    ct_ref,
    wt_ref,
    cond_v,
    val_v,
    dest,
    cz,
    cx,
    cf,
    cs,
    vf,
    hi,
    hf,
    hs,
    wf,
    load_sem,
    cz_send,
    cz_recv,
    cx_send,
    cx_recv,
    cy_send,
    cy_recv,
    vy_send,
    vy_recv,
    vz_send,
    vz_recv,
    vx_send,
    vx_recv,
    hi_send,
    hi_recv,
    hy_send,
    hy_recv,
    hz_send,
    hz_recv,
    hx_send,
    hx_recv,
    w_send,
    w_recv,
):
    ny, nx, nz = ring
    count = ny * nx * nz
    me = lax.axis_index("kgrp")
    img = lax.axis_index("img")
    y = lax.div(me, nx * nz)
    x = lax.rem(lax.div(me, nz), nx)
    z = lax.rem(me, nz)

    def at(yy, xx, zz, gg):
        return ((yy * nx + xx) * nz + zz, gg)

    def y_peer(step):
        yy = lax.rem(y + step, ny)
        return yy, at(yy, x, z, img)

    def x_peer(step):
        xx = lax.rem(x + step, nx)
        return xx, at(y, xx, z, img)

    def z_peer(step):
        zz = lax.rem(z + step, nz)
        return zz, at(y, x, zz, img)

    def img_peer(step):
        return (me, lax.rem(img + step, groups))

    def send(src, dst, send_sem, recv_sem, device):
        pltpu.make_async_remote_copy(
            src_ref=src,
            dst_ref=dst,
            send_sem=send_sem,
            recv_sem=recv_sem,
            device_id=device,
            device_id_type=MESH,
        ).start()

    load_val = pltpu.make_async_copy(val_hbm, val_v, load_sem.at[0])
    load_cond = pltpu.make_async_copy(cond_hbm, cond_v, load_sem.at[1])
    load_val.start()
    load_cond.start()

    barrier = pltpu.get_barrier_semaphore()
    peers = (
        [y_peer(s)[1] for s in range(1, ny)]
        + [z_peer(s)[1] for s in range(1, nz)]
        + [x_peer(s)[1] for s in range(1, nx)]
        + [img_peer(s) for s in range(1, groups)]
    )
    for peer in peers:
        pl.semaphore_signal(barrier, inc=1, device_id=peer, device_id_type=MESH)

    vf[y, x, z] = vec_ref[...].reshape(8, vec_ref.shape[2]).astype(vf.dtype)

    points = val_v.shape[1]
    wanted = hole_ref[0] - img * points
    lane8 = lax.broadcasted_iota(jnp.int32, (8, LANES), 1)
    lane32 = lax.broadcasted_iota(jnp.int32, (32, LANES), 1)
    load_val.wait()

    def pick(j, kept):
        tile = val_v[:, pl.ds(pl.multiple_of(j * LANES, LANES), LANES)].astype(jnp.float32)
        return kept + jnp.where(lane32 + j * LANES == wanted, tile, 0.0)

    tile = lax.fori_loop(0, points // LANES, pick, jnp.zeros((32, LANES), jnp.float32))
    tile = jnp.concatenate([tile, jnp.zeros((LANES - 32, LANES), jnp.float32)], 0)
    tile = tile.astype(jnp.bfloat16)
    chosen = jnp.ones((8, LANES), jnp.bfloat16)
    row = lax.dot_general(
        chosen, tile, (((1,), (1,)), ((), ())), preferred_element_type=jnp.float32
    )
    hi[img] = row[0:1]

    load_cond.wait()
    low = lane8 < 64
    odd = lax.rem(lax.div(lane8, 32), 2) == 1

    def relay(j, carry):
        yy = lax.div(j, nx)
        xx = lax.rem(j, nx)
        t = [
            cond_v[q, :, pl.ds(pl.multiple_of(j * LANES, LANES), LANES)].astype(jnp.float32)
            for q in range(4)
        ]
        halves = []
        for q in range(2):
            halves.append(jnp.where(low, t[q], pltpu.roll(t[q + 2], 64, 1)))
        for q in range(2):
            halves.append(jnp.where(low, pltpu.roll(t[q], 64, 1), t[q + 2]))
        for h in range(2):
            first, second = halves[2 * h], halves[2 * h + 1]
            dest[yy, xx, 2 * h] = jnp.where(odd, pltpu.roll(second, 32, 1), first).astype(
                jnp.bfloat16
            )
            dest[yy, xx, 2 * h + 1] = jnp.where(odd, second, pltpu.roll(first, 96, 1)).astype(
                jnp.bfloat16
            )
        return carry

    lax.fori_loop(0, ny * nx, relay, 0)

    def own_z(j, carry):
        yy = lax.div(j, nx)
        xx = lax.rem(j, nx)
        cz[yy, z, xx] = dest[yy, xx, z]
        return carry

    lax.fori_loop(0, ny * nx, own_z, 0)

    pl.semaphore_wait(barrier, len(peers))

    for s in range(1, groups):
        send(hi.at[img], hi.at[img], hi_send, hi_recv, img_peer(s))
    far_y = sorted(range(1, ny), key=lambda s: -min(s, ny - s))
    far_z = sorted(range(1, nz), key=lambda s: -min(s, nz - s))
    far_x = sorted(range(1, nx), key=lambda s: -min(s, nx - s))
    for s in far_y:
        send(vf.at[y, x, z], vf.at[y, x, z], vy_send, vy_recv, y_peer(s)[1])

    order = far_y + [0]
    for s in order:
        yy = lax.rem(y + s, ny)
        for t in far_z:
            zz, device = z_peer(t)
            send(dest.at[yy, :, zz], cz.at[yy, z], cz_send, cz_recv.at[s], device)

    drain(hi_recv, hi.at[pl.ds(0, groups - 1)])
    total = hi[0]
    for s in range(1, groups):
        total = total + hi[s]
    hf[y, x, z] = total

    drain(vy_recv, vf.at[pl.ds(0, ny - 1), 0, 0])
    for t in far_z:
        send(vf.at[:, x, z], vf.at[:, x, z], vz_send, vz_recv.at[t], z_peer(t)[1])
    for t in far_x:
        send(vf.at[:, x, z], vf.at[:, x, z], vx_send, vx_recv, x_peer(t)[1])
    for s in far_y:
        send(hf.at[y, x, z], hf.at[y, x, z], hy_send, hy_recv, y_peer(s)[1])

    def forward_x(s):
        yy = lax.rem(y + s, ny)
        drain(cz_recv.at[s], cz.at[yy, pl.ds(0, nz - 1)])
        for t in far_x:
            xx, device = x_peer(t)
            send(cz.at[yy, :, xx], cx.at[yy, x], cx_send, cx_recv.at[s], device)
        for zz in range(nz):
            cx[yy, x, zz] = cz[yy, zz, x]

    for s in order[: ny // 2]:
        forward_x(s)

    for t in sorted(range(1, nz), key=lambda t: min(t, nz - t)):
        zz = lax.rem(z + nz - t, nz)
        drain(vz_recv.at[t], vf.at[:, 0, 0])
        for u in far_x:
            send(vf.at[:, x, zz], vf.at[:, x, zz], vx_send, vx_recv, x_peer(u)[1])

    drain(hy_recv, hf.at[pl.ds(0, ny - 1), 0, 0])
    for t in far_z:
        send(hf.at[:, x, z], hf.at[:, x, z], hz_send, hz_recv, z_peer(t)[1])

    for s in order[ny // 2 :]:
        forward_x(s)

    def forward_y(s):
        yy, device = y_peer(s)
        drain(cx_recv.at[s], cx.at[yy, pl.ds(0, nx - 1)])
        send(cx.at[yy], cf.at[y], cy_send, cy_recv, device)

    for s in far_y[: ny // 2]:
        forward_y(s)

    drain(hz_recv, hf.at[:, 0, pl.ds(0, nz - 1)])
    for t in far_x:
        send(hf.at[:, x], hf.at[:, x], hx_send, hx_recv, x_peer(t)[1])

    for s in far_y[ny // 2 :]:
        forward_y(s)
    drain(cx_recv.at[0], cx.at[y, pl.ds(0, nx - 1)])
    cf[y] = cx[y]

    drain(vx_recv, vf.at[:, pl.ds(0, nx - 1)])
    drain(hx_recv, hf.at[:, pl.ds(0, nx - 1)])

    for d in range(count):
        hs[pl.ds(d, 1), :] = hf[d // (nx * nz), d // nz % nx, d % nz]
    holes = jnp.transpose(hs[...])
    upper = lax.broadcasted_iota(jnp.int32, (8, vf.shape[4]), 0) < 4
    for a in range(2):
        for c in range(nc):
            along = None
            across = None
            for v in range(NV):
                d = (a * NV + v) * nc + c
                piece = vf[d // (nx * nz), d // nz % nx, d % nz].astype(jnp.float32)
                real = piece * holes[a * 16 + v : a * 16 + v + 1]
                imag = piece * holes[a * 16 + 8 + v : a * 16 + 9 + v]
                along = real if along is None else along + real
                across = imag if across is None else across + imag
            across = pltpu.roll(across, 4, 0)
            weight = (along + jnp.where(upper, across, -across)) * ((NV * NC) ** -0.5)
            wf[img, a * nc + c] = weight.astype(jnp.bfloat16)

    for s in range(1, groups):
        send(wf.at[img], wf.at[img], w_send, w_recv, img_peer(s))

    drain(cy_recv, cf.at[pl.ds(0, ny - 1)])
    cs[...] = cf[...].astype(jnp.float32).reshape(cs.shape)
    for c in range(8):
        ct_ref[c] = jnp.transpose(cs[pl.ds(c, count, 8), :])

    drain(w_recv, wf.at[pl.ds(0, groups - 1)])
    wt_ref[...] = wf[...].astype(jnp.float32)

    drain(hi_send, hi.at[pl.ds(0, groups - 1)])
    drain(vy_send, vf.at[pl.ds(0, ny - 1), 0, 0])
    drain(vz_send, vf.at[:, 0, pl.ds(0, nz - 1)])
    drain(vx_send, vf.at[:, pl.ds(0, nx - 1)])
    drain(hy_send, hf.at[pl.ds(0, ny - 1), 0, 0])
    drain(hz_send, hf.at[:, 0, pl.ds(0, nz - 1)])
    drain(hx_send, hf.at[:, pl.ds(0, nx - 1)])
    drain(cz_send, cz.at[:, pl.ds(0, nz - 1)])
    drain(cx_send, cx.at[:, pl.ds(0, nx - 1)])
    drain(cy_send, cf.at[pl.ds(0, ny - 1)])
    drain(w_send, wf.at[pl.ds(0, groups - 1)])


def run_exchange(ring, groups, nc, hole, vec, cond, val, vec_type=jnp.bfloat16):
    ny, nx, nz = ring
    count = ny * nx * nz
    lanes = vec.shape[2]
    bf16, f32 = jnp.bfloat16, jnp.float32
    dma = pltpu.SemaphoreType.DMA
    vmem = pl.BlockSpec(memory_space=pltpu.VMEM)
    anywhere = pl.BlockSpec(memory_space=pltpu.HBM)
    scratch = [
        pltpu.VMEM(cond.shape, bf16),
        pltpu.VMEM(val.shape, bf16),
        pltpu.VMEM((ny, nx, nz, 8, LANES), bf16),
        pltpu.VMEM((ny, nz, nx, 8, LANES), bf16),
        pltpu.VMEM((ny, nx, nz, 8, LANES), bf16),
        pltpu.VMEM((ny, nx, nz, 8, LANES), bf16),
        pltpu.VMEM((count * 8, LANES), f32),
        pltpu.VMEM((ny, nx, nz, 8, lanes), vec_type),
        pltpu.VMEM((groups, 1, LANES), f32),
        pltpu.VMEM((ny, nx, nz, 1, LANES), f32),
        pltpu.VMEM((count, LANES), f32),
        pltpu.VMEM((groups, 2 * nc, 8, lanes), bf16),
        dma((2,)),
        dma(()),
        dma((ny,)),
        dma(()),
        dma((ny,)),
        dma(()),
        dma(()),
        dma(()),
        dma(()),
        dma(()),
        dma((nz,)),
        dma(()),
        dma(()),
        dma(()),
        dma(()),
        dma(()),
        dma(()),
        dma(()),
        dma(()),
        dma(()),
        dma(()),
        dma(()),
        dma(()),
    ]
    return pl.pallas_call(
        functools.partial(exchange, ring, groups, nc),
        out_shape=(
            jax.ShapeDtypeStruct((8, LANES, count), f32),
            jax.ShapeDtypeStruct((groups, 2 * nc, 8, lanes), f32),
        ),
        in_specs=[pl.BlockSpec(memory_space=pltpu.SMEM), vmem, anywhere, anywhere],
        out_specs=(vmem, vmem),
        scratch_shapes=scratch,
        compiler_params=pltpu.CompilerParams(
            collective_id=0, has_side_effects=True, vmem_limit_bytes=24 * 1024 * 1024
        ),
        name="exchange",
    )(hole, vec, cond, val)


COS30 = float(np.float32(jnp.bfloat16(np.cos(np.pi / 6))))
FIT = np.linalg.solve(
    np.array([[1.0, 1.0, 1.0], [1.0, 4.0, 16.0], [1.0, 9.0, 81.0]]),
    np.array([0.5, COS30 / 2, 1.0 / 3]),
)


def cosine(level):
    u = jnp.abs(level - 6.0) - 3.0
    square = u * u
    return u * (float(FIT[0]) + square * (float(FIT[1]) + square * float(FIT[2])))


def combine(ct_ref, wt_ref, kpt_ref, cell_ref, real_ref, imag_ref, table, lhs):
    bf16, f32 = jnp.bfloat16, jnp.float32

    @pl.when(pl.program_id(0) == 0)
    def _():
        kpt = kpt_ref[...].astype(f32)
        cell = cell_ref[...].astype(f32)
        kpt = jnp.concatenate([kpt, jnp.zeros((5, kpt.shape[1]), f32)], 0).astype(bf16)
        cell = jnp.concatenate([cell, jnp.zeros((5, cell.shape[1]), f32)], 0).astype(bf16)
        rows = lax.broadcasted_iota(jnp.int32, (256, 256), 0)
        columns = lax.broadcasted_iota(jnp.int32, (256, 256), 1)
        source = 2 * jnp.bitwise_and(columns, 127) + jnp.right_shift(columns, 7)
        swap = jnp.where(rows == source, 1.0, 0.0).astype(bf16)
        kpt = jnp.dot(kpt, swap, preferred_element_type=f32)
        for a in range(2):
            part = jnp.transpose(kpt[:, a * 128 : a * 128 + 128]).astype(bf16)
            turns = jnp.dot(part, cell, preferred_element_type=f32)
            turns = turns - 12.0 * jnp.floor((turns + 0.5) * (1.0 / 12.0))
            cos = cosine(turns).astype(bf16)
            shifted = turns - 3.0
            sin = cosine(jnp.where(shifted < 0.0, shifted + 12.0, shifted)).astype(bf16)
            table[a * 256 : a * 256 + 128, 0:512] = cos
            table[a * 256 : a * 256 + 128, 512:1024] = sin
            table[a * 256 + 128 : a * 256 + 256, 0:512] = -sin
            table[a * 256 + 128 : a * 256 + 256, 512:1024] = cos

    for a in range(2):
        for half in range(2):
            reals = []
            imags = []
            for c in range(NC):
                start = a * 64 + half * 16
                reals.append(ct_ref[c, start : start + 16, :])
                imags.append(ct_ref[c, start + 32 : start + 48, :])
            for s in range(4):
                out_real = None
                out_imag = None
                for c in range(NC):
                    wr = wt_ref[0, a * NC + c, s : s + 1, :]
                    wi = wt_ref[0, a * NC + c, s + 4 : s + 5, :]
                    tr = wr * reals[c] - wi * imags[c]
                    ti = wr * imags[c] + wi * reals[c]
                    out_real = tr if out_real is None else out_real + tr
                    out_imag = ti if out_imag is None else out_imag + ti
                first = s * 32 + half * 16
                lhs[first : first + 16, a * 256 : a * 256 + 128] = out_real.astype(bf16)
                lhs[first : first + 16, a * 256 + 128 : a * 256 + 256] = out_imag.astype(bf16)

    scale = 512.0**-0.5
    for part, ref in ((0, real_ref), (1, imag_ref)):
        ref[...] = (
            jnp.dot(
                lhs[...],
                table[:, part * 512 : part * 512 + 512],
                preferred_element_type=f32,
            )
            * scale
        )


def run_combine(ct, wt, kpoint_grid, image_cells):
    f32 = jnp.float32
    groups = wt.shape[0]
    rows = 4 * PTS
    return pl.pallas_call(
        combine,
        grid=(groups,),
        out_shape=(
            jax.ShapeDtypeStruct((groups * rows, 512), f32),
            jax.ShapeDtypeStruct((groups * rows, 512), f32),
        ),
        in_specs=[
            pl.BlockSpec(ct.shape, lambda i: (0, 0, 0)),
            pl.BlockSpec((1,) + wt.shape[1:], lambda i: (i, 0, 0, 0)),
            pl.BlockSpec(kpoint_grid.shape, lambda i: (0, 0)),
            pl.BlockSpec(image_cells.shape, lambda i: (0, 0)),
        ],
        out_specs=(
            pl.BlockSpec((rows, 512), lambda i: (i, 0)),
            pl.BlockSpec((rows, 512), lambda i: (i, 0)),
        ),
        scratch_shapes=[
            pltpu.VMEM((512, 1024), jnp.bfloat16),
            pltpu.VMEM((rows, 512), jnp.bfloat16),
        ],
        compiler_params=pltpu.CompilerParams(vmem_limit_bytes=24 * 1024 * 1024),
        name="combine",
    )(ct, wt, kpoint_grid, image_cells)


def shards(vectors, conduction, valence, hole_point, kpoint_grid, image_cells):
    points = conduction.shape[4]
    cond = conduction.reshape(4, 8, points)
    val = valence.reshape(32, points)
    ct, wt = run_exchange(RING, lax.axis_size("img"), NC, hole_point, vectors, cond, val)
    real, imag = run_combine(ct, wt, kpoint_grid, image_cells)
    shape = (16, 1, PTS, 512)
    return real.reshape(shape), imag.reshape(shape)


def solution(mesh):
    placed = (
        P(None, "img", "kgrp"),
        P("kgrp", None, None, "img", None),
        P("kgrp", None, None, "img", None),
        P(),
        P(),
        P(),
    )
    return jax.shard_map(
        shards,
        mesh=mesh,
        in_specs=placed,
        out_specs=(P(None, "img", "kgrp", None), P(None, "img", "kgrp", None)),
        check_vma=False,
    )
```

```python
import contextlib
import functools

import jax
import jax.numpy as jnp
import numpy as np
from jax import lax
from jax.experimental import pallas as pl
from jax.experimental.pallas import tpu as pltpu
from jax.sharding import PartitionSpec as P

MESH = pl.DeviceIdType.MESH
RING = (8, 4, 4)
NV = 8
NC = 8
LANES = 128
PTS = 32
GRANT = 67043328


def stage(name):
    return contextlib.nullcontext()


def drain(sem, ref):
    pltpu.make_async_copy(ref, ref, sem).wait()


COS30 = float(np.float32(jnp.bfloat16(np.cos(np.pi / 6))))
FIT = np.linalg.solve(
    np.array([[1.0, 1.0, 1.0], [1.0, 4.0, 16.0], [1.0, 9.0, 81.0]]),
    np.array([0.5, COS30 / 2, 1.0 / 3]),
)


def cosine(level):
    u = jnp.abs(level - 6.0) - 3.0
    square = u * u
    return u * (float(FIT[0]) + square * (float(FIT[1]) + square * float(FIT[2])))


def phases(kpt_ref, cell_ref, table):
    bf16, f32 = jnp.bfloat16, jnp.float32
    kpt = kpt_ref[...].astype(f32)
    cell = cell_ref[...].astype(f32)
    kpt = jnp.concatenate([kpt, jnp.zeros((5, kpt.shape[1]), f32)], 0).astype(bf16)
    cell = jnp.concatenate([cell, jnp.zeros((5, cell.shape[1]), f32)], 0).astype(bf16)
    rows = lax.broadcasted_iota(jnp.int32, (256, 256), 0)
    columns = lax.broadcasted_iota(jnp.int32, (256, 256), 1)
    source = 2 * jnp.bitwise_and(columns, 127) + jnp.right_shift(columns, 7)
    swap = jnp.where(rows == source, 1.0, 0.0).astype(bf16)
    kpt = jnp.dot(kpt, swap, preferred_element_type=f32)
    for a in range(2):
        part = jnp.transpose(kpt[:, a * 128 : a * 128 + 128]).astype(bf16)
        turns = jnp.dot(part, cell, preferred_element_type=f32)
        turns = turns - 12.0 * jnp.floor((turns + 0.5) * (1.0 / 12.0))
        cos = cosine(turns).astype(bf16)
        shifted = turns - 3.0
        sin = cosine(jnp.where(shifted < 0.0, shifted + 12.0, shifted)).astype(bf16)
        table[a * 256 : a * 256 + 128, 0:512] = cos
        table[a * 256 : a * 256 + 128, 512:1024] = sin
        table[a * 256 + 128 : a * 256 + 256, 0:512] = -sin
        table[a * 256 + 128 : a * 256 + 256, 512:1024] = cos


def exchange(
    ring,
    groups,
    nc,
    hole_hbm,
    vec_hbm,
    cond_hbm,
    val_hbm,
    kpt_hbm,
    cell_hbm,
    real_hbm,
    imag_hbm,
    hole_v,
    vec_v,
    kpt_v,
    cell_v,
    cond_v,
    val_v,
    dest,
    cx,
    cy,
    cf,
    cs,
    ct,
    vf,
    hi,
    hf,
    hs,
    wf,
    wt,
    table,
    lhs,
    real_v,
    imag_v,
    load_sem,
    out_sem,
    cx_send,
    cx_recv,
    cy_send,
    cy_recv,
    cz_send,
    cz_recv,
    vy_send,
    vy_recv,
    vz_send,
    vz_recv,
    vx_send,
    vx_recv,
    hi_send,
    hi_recv,
    hy_send,
    hy_recv,
    hz_send,
    hz_recv,
    hx_send,
    hx_recv,
    w_send,
    w_recv,
):
    ny, nx, nz = ring
    count = ny * nx * nz
    me = lax.axis_index("kgrp")
    img = lax.axis_index("img")
    y = lax.div(me, nx * nz)
    x = lax.rem(lax.div(me, nz), nx)
    z = lax.rem(me, nz)
    bf16, f32 = jnp.bfloat16, jnp.float32

    def at(yy, xx, zz, gg):
        return ((yy * nx + xx) * nz + zz, gg)

    def y_peer(step):
        yy = lax.rem(y + step, ny)
        return yy, at(yy, x, z, img)

    def x_peer(step):
        xx = lax.rem(x + step, nx)
        return xx, at(y, xx, z, img)

    def z_peer(step):
        zz = lax.rem(z + step, nz)
        return zz, at(y, x, zz, img)

    def img_peer(step):
        return (me, jnp.bitwise_xor(img, step))

    def send(src, dst, send_sem, recv_sem, device):
        pltpu.make_async_remote_copy(
            src_ref=src,
            dst_ref=dst,
            send_sem=send_sem,
            recv_sem=recv_sem,
            device_id=device,
            device_id_type=MESH,
        ).start()

    far_y = sorted(range(1, ny), key=lambda s: -min(s, ny - s))
    far_z = sorted(range(1, nz), key=lambda s: -min(s, nz - s))
    far_x = sorted(range(1, nx), key=lambda s: -min(s, nx - s))
    far_g = list(range(groups - 1, 0, -1))
    order = far_z + [0]

    barrier = pltpu.get_barrier_semaphore()
    peers = (
        [y_peer(s)[1] for s in far_y]
        + [z_peer(s)[1] for s in far_z]
        + [x_peer(s)[1] for s in far_x]
        + [img_peer(s) for s in far_g]
    )
    load_vec = pltpu.make_async_copy(vec_hbm, vec_v, load_sem.at[2])
    load_hole = pltpu.make_async_copy(hole_hbm, hole_v, load_sem.at[3])
    load_val = pltpu.make_async_copy(val_hbm, val_v, load_sem.at[0])
    load_cond = pltpu.make_async_copy(cond_hbm, cond_v, load_sem.at[1])
    load_kpt = pltpu.make_async_copy(kpt_hbm, kpt_v, load_sem.at[4])
    load_cell = pltpu.make_async_copy(cell_hbm, cell_v, load_sem.at[5])
    for load in (load_vec, load_hole, load_val, load_cond, load_kpt, load_cell):
        load.start()
    with stage("signal"):
        for peer in peers:
            pl.semaphore_signal(barrier, inc=1, device_id=peer, device_id_type=MESH)

    with stage("pack"):
        load_vec.wait()
        vf[y, x, z] = vec_v[...].reshape(8, vec_v.shape[2]).astype(vf.dtype)

    with stage("pick"):
        points = val_v.shape[1]
        load_hole.wait()
        wanted = hole_v[...] - img * points
        lane8 = lax.broadcasted_iota(jnp.int32, (8, LANES), 1)
        lane32 = lax.broadcasted_iota(jnp.int32, (32, LANES), 1)
        load_val.wait()

        def pick(j, kept):
            tile = val_v[:, pl.ds(pl.multiple_of(j * LANES, LANES), LANES)]
            return kept + jnp.where(lane32 + j * LANES == wanted, tile.astype(f32), 0.0)

        tile = lax.fori_loop(
            0, points // LANES, pick, jnp.zeros((32, LANES), f32), unroll=8
        )
        tile = jnp.concatenate([tile, jnp.zeros((LANES - 32, LANES), f32)], 0)
        tile = tile.astype(bf16)
        chosen = jnp.ones((8, LANES), bf16)
        row = lax.dot_general(
            chosen, tile, (((1,), (1,)), ((), ())), preferred_element_type=f32
        )
        hi[img] = row[0:1]

    low = lane8 < 64
    odd = lax.rem(lax.div(lane8, 32), 2) == 1

    def relay(j, carry):
        yy = lax.div(j, nx)
        xx = lax.rem(j, nx)
        column = pl.ds(pl.multiple_of(j * LANES, LANES), LANES)
        t = [cond_v[q, :, column].astype(f32) for q in range(4)]
        halves = []
        for q in range(2):
            halves.append(jnp.where(low, t[q], pltpu.roll(t[q + 2], 64, 1)))
        for q in range(2):
            halves.append(jnp.where(low, pltpu.roll(t[q], 64, 1), t[q + 2]))
        for h in range(2):
            first, second = halves[2 * h], halves[2 * h + 1]
            dest[yy, xx, 2 * h] = jnp.where(odd, pltpu.roll(second, 32, 1), first).astype(bf16)
            dest[yy, xx, 2 * h + 1] = jnp.where(odd, second, pltpu.roll(first, 96, 1)).astype(bf16)
        return carry

    with stage("relay"):
        load_cond.wait()
        lax.fori_loop(0, ny * nx, relay, 0, unroll=16)
        for zz in range(nz):
            for yy in range(ny):
                cx[zz, x, yy] = dest[yy, x, zz]

    with stage("barrier"):
        pl.semaphore_wait(barrier, len(peers))

    for s in far_y:
        send(vf.at[y, x, z], vf.at[y, x, z], vy_send, vy_recv, y_peer(s)[1])
    for s in far_g:
        send(hi.at[img], hi.at[img], hi_send, hi_recv, img_peer(s))
    for s in order:
        zz = lax.rem(z + s, nz)
        for t in far_x:
            xx, device = x_peer(t)
            send(dest.at[:, xx, zz], cx.at[zz, x], cx_send, cx_recv.at[s], device)

    with stage("phases"):
        load_kpt.wait()
        load_cell.wait()
        if count == LANES:
            phases(kpt_v, cell_v, table)

    with stage("hole_img"):
        drain(hi_recv, hi.at[pl.ds(0, groups - 1)])
    total = hi[0]
    for s in range(1, groups):
        total = total + hi[s]
    hf[y, x, z] = total

    def wait_x(s):
        zz = lax.rem(z + s, nz)
        with stage(f"cx{s}"):
            drain(cx_recv.at[s], cx.at[zz, pl.ds(0, nx - 1)])

    def forward_y(s):
        zz = lax.rem(z + s, nz)
        for t in far_y:
            yy, device = y_peer(t)
            send(cx.at[zz, :, yy], cy.at[zz, y], cy_send, cy_recv.at[s], device)
        for xx in range(nx):
            cy[zz, y, xx] = cx[zz, xx, y]

    wait_x(order[0])
    for s in far_y:
        send(hf.at[y, x, z], hf.at[y, x, z], hy_send, hy_recv, y_peer(s)[1])
    forward_y(order[0])
    for s in order[1:]:
        wait_x(s)
        forward_y(s)

    with stage("vec_y"):
        drain(vy_recv, vf.at[pl.ds(0, ny - 1), 0, 0])
    for t in far_z:
        send(vf.at[:, x, z], vf.at[:, x, z], vz_send, vz_recv.at[t], z_peer(t)[1])
    for t in far_x:
        send(vf.at[:, x, z], vf.at[:, x, z], vx_send, vx_recv, x_peer(t)[1])

    with stage("hole_y"):
        drain(hy_recv, hf.at[pl.ds(0, ny - 1), 0, 0])
    for t in far_z:
        send(hf.at[:, x, z], hf.at[:, x, z], hz_send, hz_recv, z_peer(t)[1])

    def forward_v(t):
        zz = lax.rem(z + nz - t, nz)
        with stage(f"vec_z{t}"):
            drain(vz_recv.at[t], vf.at[:, 0, 0])
        for u in far_x:
            send(vf.at[:, x, zz], vf.at[:, x, zz], vx_send, vx_recv, x_peer(u)[1])

    def forward_z(s):
        zz, device = z_peer(s)
        with stage(f"cy{s}"):
            drain(cy_recv.at[s], cy.at[zz, pl.ds(0, ny - 1)])
        send(cy.at[zz], cf.at[:, :, z], cz_send, cz_recv, device)

    near_z = far_z[::-1]
    for t in near_z[:-1]:
        forward_v(t)
    for s in far_z[:2]:
        forward_z(s)
    forward_v(near_z[-1])
    for s in far_z[2:]:
        forward_z(s)

    with stage("hole_z"):
        drain(hz_recv, hf.at[:, 0, pl.ds(0, nz - 1)])
    for t in far_x:
        send(hf.at[:, x], hf.at[:, x], hx_send, hx_recv, x_peer(t)[1])

    with stage("cy0"):
        drain(cy_recv.at[0], cy.at[z, pl.ds(0, ny - 1)])
        for yy in range(ny):
            for xx in range(nx):
                cf[yy, xx, z] = cy[z, yy, xx]

    with stage("vec_x"):
        drain(vx_recv, vf.at[:, pl.ds(0, nx - 1)])
    with stage("hole_x"):
        drain(hx_recv, hf.at[:, pl.ds(0, nx - 1)])

    with stage("weights"):
        for d in range(count):
            hs[pl.ds(d, 1), :] = hf[d // (nx * nz), d // nz % nx, d % nz]
        holes = jnp.transpose(hs[...])
        upper = lax.broadcasted_iota(jnp.int32, (8, vf.shape[4]), 0) < 4
        for a in range(2):
            for c in range(nc):
                along = None
                across = None
                for v in range(NV):
                    d = (a * NV + v) * nc + c
                    piece = vf[d // (nx * nz), d // nz % nx, d % nz].astype(f32)
                    real = piece * holes[a * 16 + v : a * 16 + v + 1]
                    imag = piece * holes[a * 16 + 8 + v : a * 16 + 9 + v]
                    along = real if along is None else along + real
                    across = imag if across is None else across + imag
                across = pltpu.roll(across, 4, 0)
                weight = (along + jnp.where(upper, across, -across)) * ((NV * NC) ** -0.5)
                wf[img, a * nc + c] = weight.astype(bf16)

    with stage("cz"):
        drain(cz_recv, cf.at[:, :, pl.ds(0, nz - 1)])
    for s in far_g:
        send(wf.at[img], wf.at[img], w_send, w_recv.at[s], img_peer(s))
    with stage("turn"):
        cs[...] = cf[...].astype(f32).reshape(cs.shape)
        for c in range(8):
            ct[c] = jnp.transpose(cs[pl.ds(c, count, 8), :])

    def products(step):
        group = jnp.bitwise_xor(img, step)
        wt[...] = wf[group].astype(f32)
        for a in range(2):
            for half in range(2):
                reals = []
                imags = []
                for c in range(nc):
                    start = a * 64 + half * 16
                    reals.append(ct[c, start : start + 16, :])
                    imags.append(ct[c, start + 32 : start + 48, :])
                for s in range(4):
                    out_real = None
                    out_imag = None
                    for c in range(nc):
                        wr = wt[a * nc + c, s : s + 1, :]
                        wi = wt[a * nc + c, s + 4 : s + 5, :]
                        tr = wr * reals[c] - wi * imags[c]
                        ti = wr * imags[c] + wi * reals[c]
                        out_real = tr if out_real is None else out_real + tr
                        out_imag = ti if out_imag is None else out_imag + ti
                    first = step * 128 + s * 32 + half * 16
                    left = a * 2 * count
                    lhs[first : first + 16, left : left + count] = out_real.astype(bf16)
                    lhs[first : first + 16, left + count : left + 2 * count] = out_imag.astype(bf16)

    def finish(first, last):
        rows = slice(first * 128, last * 128)
        outs = []
        for part, (held, out) in enumerate(((real_v, real_hbm), (imag_v, imag_hbm))):
            held[rows, :] = jnp.dot(
                lhs[rows, :],
                table[0 : 4 * count, part * 512 : part * 512 + 512],
                preferred_element_type=f32,
            ) * (512.0**-0.5)
            for step in range(first, last):
                group = jnp.bitwise_xor(img, step)
                outs.append(
                    pltpu.make_async_copy(
                        held.at[pl.ds(step * 128, 128)],
                        out.at[pl.ds(pl.multiple_of(group * 128, 128), 128)],
                        out_sem.at[part, step],
                    )
                )
                outs[-1].start()
        return outs

    with stage("own"):
        products(0)
        outs = finish(0, 1)
    for s in far_g[::-1]:
        with stage(f"wimg{s}"):
            drain(w_recv.at[s], wf.at[0])
        with stage("products"):
            products(s)
    with stage("finish"):
        outs = outs + finish(1, groups)

    with stage("sends"):
        drain(hi_send, hi.at[pl.ds(0, groups - 1)])
        drain(vy_send, vf.at[pl.ds(0, ny - 1), 0, 0])
        drain(vz_send, vf.at[:, 0, pl.ds(0, nz - 1)])
        drain(vx_send, vf.at[:, pl.ds(0, nx - 1)])
        drain(hy_send, hf.at[pl.ds(0, ny - 1), 0, 0])
        drain(hz_send, hf.at[:, 0, pl.ds(0, nz - 1)])
        drain(hx_send, hf.at[:, pl.ds(0, nx - 1)])
        drain(cx_send, cx.at[:, pl.ds(0, nx - 1)])
        drain(cy_send, cy.at[:, pl.ds(0, ny - 1)])
        drain(cz_send, cf.at[:, :, pl.ds(0, nz - 1)])
        drain(w_send, wf.at[pl.ds(0, groups - 1)])
    with stage("outs"):
        for out in outs:
            out.wait()


def run_exchange(ring, groups, nc, hole, vec, cond, val, kpt, cell, vec_type=jnp.bfloat16):
    ny, nx, nz = ring
    count = ny * nx * nz
    lanes = vec.shape[2]
    bf16, f32, i32 = jnp.bfloat16, jnp.float32, jnp.int32
    dma = pltpu.SemaphoreType.DMA
    rows = groups * 4 * PTS
    anywhere = pl.BlockSpec(memory_space=pltpu.HBM)
    scratch = [
        pltpu.VMEM(hole.shape, i32),
        pltpu.VMEM(vec.shape, f32),
        pltpu.VMEM(kpt.shape, i32),
        pltpu.VMEM(cell.shape, i32),
        pltpu.VMEM(cond.shape, bf16),
        pltpu.VMEM(val.shape, bf16),
        pltpu.VMEM((ny, nx, nz, 8, LANES), bf16),
        pltpu.VMEM((nz, nx, ny, 8, LANES), bf16),
        pltpu.VMEM((nz, ny, nx, 8, LANES), bf16),
        pltpu.VMEM((ny, nx, nz, 8, LANES), bf16),
        pltpu.VMEM((count * 8, LANES), f32),
        pltpu.VMEM((8, LANES, count), f32),
        pltpu.VMEM((ny, nx, nz, 8, lanes), vec_type),
        pltpu.VMEM((groups, 1, LANES), f32),
        pltpu.VMEM((ny, nx, nz, 1, LANES), f32),
        pltpu.VMEM((count, LANES), f32),
        pltpu.VMEM((groups, 2 * nc, 8, lanes), bf16),
        pltpu.VMEM((2 * nc, 8, lanes), f32),
        pltpu.VMEM((512, 1024), bf16),
        pltpu.VMEM((rows, 4 * count), bf16),
        pltpu.VMEM((rows, 512), f32),
        pltpu.VMEM((rows, 512), f32),
        dma((6,)),
        dma((2, groups)),
        dma(()),
        dma((nz,)),
        dma(()),
        dma((nz,)),
        dma(()),
        dma(()),
        dma(()),
        dma(()),
        dma(()),
        dma((nz,)),
        dma(()),
        dma(()),
        dma(()),
        dma(()),
        dma(()),
        dma(()),
        dma(()),
        dma(()),
        dma(()),
        dma(()),
        dma(()),
        dma((groups,)),
    ]
    return pl.pallas_call(
        functools.partial(exchange, ring, groups, nc),
        out_shape=(
            jax.ShapeDtypeStruct((rows, 512), f32),
            jax.ShapeDtypeStruct((rows, 512), f32),
        ),
        in_specs=[anywhere] * 6,
        out_specs=(anywhere, anywhere),
        scratch_shapes=scratch,
        compiler_params=pltpu.CompilerParams(
            collective_id=0, has_side_effects=True, vmem_limit_bytes=GRANT
        ),
        name="exchange",
    )(hole, vec, cond, val, kpt, cell)


def shards(vectors, conduction, valence, hole_point, kpoint_grid, image_cells):
    points = conduction.shape[4]
    cond = conduction.reshape(4, 8, points)
    val = valence.reshape(32, points)
    real, imag = run_exchange(
        RING,
        lax.axis_size("img"),
        NC,
        hole_point.reshape(1, 1),
        vectors,
        cond,
        val,
        kpoint_grid,
        image_cells,
    )
    shape = (16, 1, PTS, 512)
    return real.reshape(shape), imag.reshape(shape)


def solution(mesh):
    placed = (
        P(None, "img", "kgrp"),
        P("kgrp", None, None, "img", None),
        P("kgrp", None, None, "img", None),
        P(),
        P(),
        P(),
    )
    return jax.shard_map(
        shards,
        mesh=mesh,
        in_specs=placed,
        out_specs=(P(None, "img", "kgrp", None), P(None, "img", "kgrp", None)),
        check_vma=False,
    )
```

```python
import contextlib
import functools

import jax
import jax.numpy as jnp
import numpy as np
from jax import lax
from jax.experimental import pallas as pl
from jax.experimental.pallas import tpu as pltpu
from jax.sharding import PartitionSpec as P

MESH = pl.DeviceIdType.MESH
RING = (8, 4, 4)
NV = 8
NC = 8
LANES = 128
PTS = 32
GRANT = 24 * 1024 * 1024


def stage(name):
    return contextlib.nullcontext()


def drain(sem, ref):
    pltpu.make_async_copy(ref, ref, sem).wait()


COS30 = float(np.float32(jnp.bfloat16(np.cos(np.pi / 6))))
FIT = np.linalg.solve(
    np.array([[1.0, 1.0, 1.0], [1.0, 4.0, 16.0], [1.0, 9.0, 81.0]]),
    np.array([0.5, COS30 / 2, 1.0 / 3]),
)


def cosine(level):
    u = jnp.abs(level - 6.0) - 3.0
    square = u * u
    return u * (float(FIT[0]) + square * (float(FIT[1]) + square * float(FIT[2])))


def phases(kpt_ref, cell_ref, table):
    bf16, f32 = jnp.bfloat16, jnp.float32
    kpt = kpt_ref[...].astype(f32)
    cell = cell_ref[...].astype(f32)
    kpt = jnp.concatenate([kpt, jnp.zeros((5, kpt.shape[1]), f32)], 0).astype(bf16)
    cell = jnp.concatenate([cell, jnp.zeros((5, cell.shape[1]), f32)], 0).astype(bf16)
    rows = lax.broadcasted_iota(jnp.int32, (256, 256), 0)
    columns = lax.broadcasted_iota(jnp.int32, (256, 256), 1)
    source = 2 * jnp.bitwise_and(columns, 127) + jnp.right_shift(columns, 7)
    swap = jnp.where(rows == source, 1.0, 0.0).astype(bf16)
    kpt = jnp.dot(kpt, swap, preferred_element_type=f32)
    for a in range(2):
        part = jnp.transpose(kpt[:, a * 128 : a * 128 + 128]).astype(bf16)
        turns = jnp.dot(part, cell, preferred_element_type=f32)
        turns = turns - 12.0 * jnp.floor((turns + 0.5) * (1.0 / 12.0))
        cos = cosine(turns).astype(bf16)
        shifted = turns - 3.0
        sin = cosine(jnp.where(shifted < 0.0, shifted + 12.0, shifted)).astype(bf16)
        table[a * 256 : a * 256 + 128, 0:512] = cos
        table[a * 256 : a * 256 + 128, 512:1024] = sin
        table[a * 256 + 128 : a * 256 + 256, 0:512] = -sin
        table[a * 256 + 128 : a * 256 + 256, 512:1024] = cos


def exchange(
    ring,
    groups,
    nc,
    hole_hbm,
    vec_hbm,
    cond_hbm,
    val_hbm,
    kpt_hbm,
    cell_hbm,
    lhs,
    table,
    hole_v,
    vec_v,
    kpt_v,
    cell_v,
    cond_v,
    val_v,
    dest,
    cx,
    cy,
    cf,
    cs,
    ct,
    vf,
    hy,
    hz,
    hq,
    hw,
    hs,
    wf,
    wt,
    load_sem,
    cx_send,
    cx_recv,
    cy_send,
    cy_recv,
    cz_send,
    cz_recv,
    vy_send,
    vy_recv,
    vz_send,
    vz_recv,
    vx_send,
    vx_recv,
    hy_send,
    hy_recv,
    hz_send,
    hz_recv,
    hx_send,
    hx_recv,
    w_send,
    w_recv,
):
    ny, nx, nz = ring
    count = ny * nx * nz
    me = lax.axis_index("kgrp")
    img = lax.axis_index("img")
    y = lax.div(me, nx * nz)
    x = lax.rem(lax.div(me, nz), nx)
    z = lax.rem(me, nz)
    bf16, f32 = jnp.bfloat16, jnp.float32

    def at(yy, xx, zz, gg):
        return ((yy * nx + xx) * nz + zz, gg)

    def y_peer(step):
        yy = lax.rem(y + step, ny)
        return yy, at(yy, x, z, img)

    def x_peer(step):
        xx = lax.rem(x + step, nx)
        return xx, at(y, xx, z, img)

    def z_peer(step):
        zz = lax.rem(z + step, nz)
        return zz, at(y, x, zz, img)

    def img_peer(step):
        return (me, jnp.bitwise_xor(img, step))

    def corner(step, flip):
        return at(y, lax.rem(x + step, nx), z, jnp.bitwise_xor(img, flip))

    def send(src, dst, send_sem, recv_sem, device):
        pltpu.make_async_remote_copy(
            src_ref=src,
            dst_ref=dst,
            send_sem=send_sem,
            recv_sem=recv_sem,
            device_id=device,
            device_id_type=MESH,
        ).start()

    far_y = sorted(range(1, ny), key=lambda s: -min(s, ny - s))
    far_z = sorted(range(1, nz), key=lambda s: -min(s, nz - s))
    far_x = sorted(range(1, nx), key=lambda s: -min(s, nx - s))
    far_g = list(range(groups - 1, 0, -1))
    order = far_z + [0]

    barrier = pltpu.get_barrier_semaphore()
    peers = (
        [y_peer(s)[1] for s in far_y]
        + [z_peer(s)[1] for s in far_z]
        + [x_peer(s)[1] for s in far_x]
        + [img_peer(s) for s in far_g]
        + [corner(s, t) for s in far_x for t in far_g]
    )
    with stage("signal"):
        for peer in peers:
            pl.semaphore_signal(barrier, inc=1, device_id=peer, device_id_type=MESH)
    load_vec = pltpu.make_async_copy(vec_hbm, vec_v, load_sem.at[2])
    load_hole = pltpu.make_async_copy(hole_hbm, hole_v, load_sem.at[3])
    load_val = pltpu.make_async_copy(val_hbm, val_v, load_sem.at[0])
    load_cond = pltpu.make_async_copy(cond_hbm, cond_v, load_sem.at[1])
    load_kpt = pltpu.make_async_copy(kpt_hbm, kpt_v, load_sem.at[4])
    load_cell = pltpu.make_async_copy(cell_hbm, cell_v, load_sem.at[5])
    for load in (load_vec, load_hole, load_val, load_cond, load_kpt, load_cell):
        load.start()

    with stage("pack"):
        load_vec.wait()
        vf[y, x, z] = vec_v[...].reshape(8, vec_v.shape[2]).astype(vf.dtype)

    with stage("pick"):
        points = val_v.shape[1]
        load_hole.wait()
        wanted = hole_v[...] - img * points
        lane8 = lax.broadcasted_iota(jnp.int32, (8, LANES), 1)
        lane32 = lax.broadcasted_iota(jnp.int32, (32, LANES), 1)
        load_val.wait()

        def pick(j, kept):
            tile = val_v[:, pl.ds(pl.multiple_of(j * LANES, LANES), LANES)]
            return kept + jnp.where(lane32 + j * LANES == wanted, tile.astype(f32), 0.0)

        tile = lax.fori_loop(
            0, points // LANES, pick, jnp.zeros((32, LANES), f32), unroll=8
        )
        tile = jnp.concatenate([tile, jnp.zeros((LANES - 32, LANES), f32)], 0)
        tile = pltpu.roll(tile, z * 32, 0).astype(bf16)
        chosen = jnp.ones((8, LANES), bf16)
        row = lax.dot_general(
            chosen, tile, (((1,), (1,)), ((), ())), preferred_element_type=f32
        )
        hy[y] = row[0:1]

    low = lane8 < 64
    odd = lax.rem(lax.div(lane8, 32), 2) == 1

    def relay(j, carry):
        yy = lax.div(j, nx)
        xx = lax.rem(j, nx)
        column = pl.ds(pl.multiple_of(j * LANES, LANES), LANES)
        t = [cond_v[q, :, column].astype(f32) for q in range(4)]
        halves = []
        for q in range(2):
            halves.append(jnp.where(low, t[q], pltpu.roll(t[q + 2], 64, 1)))
        for q in range(2):
            halves.append(jnp.where(low, pltpu.roll(t[q], 64, 1), t[q + 2]))
        for h in range(2):
            first, second = halves[2 * h], halves[2 * h + 1]
            dest[yy, xx, 2 * h] = jnp.where(odd, pltpu.roll(second, 32, 1), first).astype(bf16)
            dest[yy, xx, 2 * h + 1] = jnp.where(odd, second, pltpu.roll(first, 96, 1)).astype(bf16)
        return carry

    with stage("relay"):
        load_cond.wait()
        lax.fori_loop(0, ny * nx, relay, 0, unroll=16)
        for zz in range(nz):
            for yy in range(ny):
                cx[zz, x, yy] = dest[yy, x, zz]

    with stage("barrier"):
        pl.semaphore_wait(barrier, len(peers))

    for s in far_y:
        send(vf.at[y, x, z], vf.at[y, x, z], vy_send, vy_recv, y_peer(s)[1])
    for s in far_y:
        send(hy.at[y], hy.at[y], hy_send, hy_recv, y_peer(s)[1])
    for s in order:
        zz = lax.rem(z + s, nz)
        for t in far_x:
            xx, device = x_peer(t)
            send(dest.at[:, xx, zz], cx.at[zz, x], cx_send, cx_recv.at[s], device)

    with stage("phases"):
        load_kpt.wait()
        load_cell.wait()
        if count == LANES:
            phases(kpt_v, cell_v, table)

    def wait_x(s):
        zz = lax.rem(z + s, nz)
        with stage(f"cx{s}"):
            drain(cx_recv.at[s], cx.at[zz, pl.ds(0, nx - 1)])

    def forward_y(s):
        zz = lax.rem(z + s, nz)
        for t in far_y:
            yy, device = y_peer(t)
            send(cx.at[zz, :, yy], cy.at[zz, y], cy_send, cy_recv.at[s], device)
        for xx in range(nx):
            cy[zz, y, xx] = cx[zz, xx, y]

    for s in order:
        wait_x(s)
        forward_y(s)

    with stage("vec_y"):
        drain(vy_recv, vf.at[pl.ds(0, ny - 1), 0, 0])
    for t in far_z:
        send(vf.at[:, x, z], vf.at[:, x, z], vz_send, vz_recv.at[t], z_peer(t)[1])
    for t in far_x:
        send(vf.at[:, x, z], vf.at[:, x, z], vx_send, vx_recv, x_peer(t)[1])

    with stage("hole_y"):
        drain(hy_recv, hy.at[pl.ds(0, ny - 1)])
    for t in far_z:
        send(hy, hz.at[z], hz_send, hz_recv, z_peer(t)[1])
    hz[z] = hy[...]

    def forward_v(t):
        zz = lax.rem(z + nz - t, nz)
        with stage(f"vec_z{t}"):
            drain(vz_recv.at[t], vf.at[:, 0, 0])
        for u in far_x:
            send(vf.at[:, x, zz], vf.at[:, x, zz], vx_send, vx_recv, x_peer(u)[1])

    def forward_z(s):
        zz, device = z_peer(s)
        with stage(f"cy{s}"):
            drain(cy_recv.at[s], cy.at[zz, pl.ds(0, ny - 1)])
        send(cy.at[zz], cf.at[:, :, z], cz_send, cz_recv, device)

    near_z = far_z[::-1]
    for t in near_z[:-1]:
        forward_v(t)
    for s in far_z[:2]:
        forward_z(s)
    forward_v(near_z[-1])

    with stage("hole_z"):
        drain(hz_recv, hz.at[pl.ds(0, nz - 1)])
        packed = hz[0]
        for t in range(1, nz):
            packed = packed + hz[t]
        hq[x, img] = packed
    for s in far_z[2:]:
        forward_z(s)
    for s in far_x:
        send(hq.at[x, img], hq.at[x, img], hx_send, hx_recv, x_peer(s)[1])
        for t in far_g:
            send(hq.at[x, img], hq.at[x, img], hx_send, hx_recv, corner(s, t))
    for t in far_g:
        send(hq.at[x, img], hq.at[x, img], hx_send, hx_recv, img_peer(t))

    def wait_holes(sem):
        pltpu.make_async_copy(hw, hw, sem).wait()

    with stage("cy0"):
        drain(cy_recv.at[0], cy.at[z, pl.ds(0, ny - 1)])
        for yy in range(ny):
            for xx in range(nx):
                cf[yy, xx, z] = cy[z, yy, xx]

    with stage("vec_x"):
        drain(vx_recv, vf.at[:, pl.ds(0, nx - 1)])
    with stage("hole_x"):
        wait_holes(hx_recv)

    with stage("weights"):
        for xx in range(nx):
            part = hq[xx, 0]
            for t in range(1, groups):
                part = part + hq[xx, t]
            part = part.reshape(ny, LANES)
            for zz in range(nz):
                turned = part if zz == 0 else pltpu.roll(part, LANES - 32 * zz, 1)
                hs[pl.ds(xx * nz + zz, ny, nx * nz), :] = turned
        holes = jnp.transpose(hs[...])
        upper = lax.broadcasted_iota(jnp.int32, (8, vf.shape[4]), 0) < 4
        for a in range(2):
            for c in range(nc):
                along = None
                across = None
                for v in range(NV):
                    d = (a * NV + v) * nc + c
                    piece = vf[d // (nx * nz), d // nz % nx, d % nz].astype(f32)
                    real = piece * holes[a * 16 + v : a * 16 + v + 1]
                    imag = piece * holes[a * 16 + 8 + v : a * 16 + 9 + v]
                    along = real if along is None else along + real
                    across = imag if across is None else across + imag
                across = pltpu.roll(across, 4, 0)
                weight = (along + jnp.where(upper, across, -across)) * ((NV * NC) ** -0.5)
                wf[img, a * nc + c] = weight.astype(bf16)

    for s in far_g[::-1]:
        send(wf.at[img], wf.at[img], w_send, w_recv.at[s], img_peer(s))
    with stage("cz"):
        drain(cz_recv, cf.at[:, :, pl.ds(0, nz - 1)])
    with stage("turn"):
        cs[...] = cf[...].astype(f32).reshape(cs.shape)
        for c in range(8):
            ct[c] = jnp.transpose(cs[pl.ds(c, count, 8), :])

    def products(step):
        group = jnp.bitwise_xor(img, step)
        wt[...] = wf[group].astype(f32)
        for a in range(2):
            for half in range(2):
                reals = []
                imags = []
                for c in range(nc):
                    start = a * 64 + half * 16
                    reals.append(ct[c, start : start + 16, :])
                    imags.append(ct[c, start + 32 : start + 48, :])
                for s in range(4):
                    out_real = None
                    out_imag = None
                    for c in range(nc):
                        wr = wt[a * nc + c, s : s + 1, :]
                        wi = wt[a * nc + c, s + 4 : s + 5, :]
                        tr = wr * reals[c] - wi * imags[c]
                        ti = wr * imags[c] + wi * reals[c]
                        out_real = tr if out_real is None else out_real + tr
                        out_imag = ti if out_imag is None else out_imag + ti
                    first = pl.multiple_of(group * 128 + (s * 32 + half * 16), 16)
                    left = a * 2 * count
                    here = pl.ds(first, 16)
                    lhs[here, left : left + count] = out_real.astype(bf16)
                    lhs[here, left + count : left + 2 * count] = out_imag.astype(bf16)

    with stage("own"):
        products(0)
    for s in far_g[::-1]:
        with stage(f"wimg{s}"):
            drain(w_recv.at[s], wf.at[0])
        with stage("products"):
            products(s)

    with stage("sends"):
        drain(vy_send, vf.at[pl.ds(0, ny - 1), 0, 0])
        drain(vz_send, vf.at[:, 0, pl.ds(0, nz - 1)])
        drain(vx_send, vf.at[:, pl.ds(0, nx - 1)])
        drain(hy_send, hy.at[pl.ds(0, ny - 1)])
        drain(hz_send, hz.at[pl.ds(0, nz - 1)])
        wait_holes(hx_send)
        drain(cx_send, cx.at[:, pl.ds(0, nx - 1)])
        drain(cy_send, cy.at[:, pl.ds(0, ny - 1)])
        drain(cz_send, cf.at[:, :, pl.ds(0, nz - 1)])
        drain(w_send, wf.at[pl.ds(0, groups - 1)])


def run_exchange(ring, groups, nc, hole, vec, cond, val, kpt, cell, vec_type=jnp.bfloat16):
    ny, nx, nz = ring
    count = ny * nx * nz
    lanes = vec.shape[2]
    bf16, f32, i32 = jnp.bfloat16, jnp.float32, jnp.int32
    dma = pltpu.SemaphoreType.DMA
    rows = groups * 4 * PTS
    anywhere = pl.BlockSpec(memory_space=pltpu.HBM)
    vmem = pl.BlockSpec(memory_space=pltpu.VMEM)
    scratch = [
        pltpu.VMEM(hole.shape, i32),
        pltpu.VMEM(vec.shape, f32),
        pltpu.VMEM(kpt.shape, i32),
        pltpu.VMEM(cell.shape, i32),
        pltpu.VMEM(cond.shape, bf16),
        pltpu.VMEM(val.shape, bf16),
        pltpu.VMEM((ny, nx, nz, 8, LANES), bf16),
        pltpu.VMEM((nz, nx, ny, 8, LANES), bf16),
        pltpu.VMEM((nz, ny, nx, 8, LANES), bf16),
        pltpu.VMEM((ny, nx, nz, 8, LANES), bf16),
        pltpu.VMEM((count * 8, LANES), f32),
        pltpu.VMEM((8, LANES, count), f32),
        pltpu.VMEM((ny, nx, nz, 8, lanes), vec_type),
        pltpu.VMEM((ny, 1, LANES), f32),
        pltpu.VMEM((nz, ny, 1, LANES), f32),
        pltpu.VMEM((nx, groups, ny, 1, LANES), f32),
        pltpu.VMEM((nx * groups - 1, ny, 1, LANES), f32),
        pltpu.VMEM((count, LANES), f32),
        pltpu.VMEM((groups, 2 * nc, 8, lanes), bf16),
        pltpu.VMEM((2 * nc, 8, lanes), f32),
        dma((6,)),
        dma(()),
        dma((nz,)),
        dma(()),
        dma((nz,)),
        dma(()),
        dma(()),
        dma(()),
        dma(()),
        dma(()),
        dma((nz,)),
        dma(()),
        dma(()),
        dma(()),
        dma(()),
        dma(()),
        dma(()),
        dma(()),
        dma(()),
        dma(()),
        dma((groups,)),
    ]
    return pl.pallas_call(
        functools.partial(exchange, ring, groups, nc),
        out_shape=(
            jax.ShapeDtypeStruct((rows, 4 * count), bf16),
            jax.ShapeDtypeStruct((512, 1024), bf16),
        ),
        in_specs=[anywhere] * 6,
        out_specs=(vmem, vmem),
        scratch_shapes=scratch,
        compiler_params=pltpu.CompilerParams(
            collective_id=0, has_side_effects=True, vmem_limit_bytes=GRANT
        ),
        name="exchange",
    )(hole, *(pltpu.with_memory_space_constraint(v, pltpu.HBM) for v in (vec, cond, val, kpt, cell)))


def combine(lhs, table, real_ref, imag_ref):
    half = real_ref.shape[1]
    scale = 512.0**-0.5
    for part, ref in ((0, real_ref), (1, imag_ref)):
        start = pl.multiple_of(part * 512 + pl.program_id(0) * half, half)
        ref[...] = (
            jnp.dot(lhs[...], table[:, pl.ds(start, half)], preferred_element_type=jnp.float32)
            * scale
        )


def run_combine(lhs, table):
    rows = lhs.shape[0]
    vmem = pl.BlockSpec(memory_space=pltpu.VMEM)
    block = pl.BlockSpec((rows, 256), lambda i: (0, i))
    return pl.pallas_call(
        combine,
        grid=(2,),
        out_shape=(
            jax.ShapeDtypeStruct((rows, 512), jnp.float32),
            jax.ShapeDtypeStruct((rows, 512), jnp.float32),
        ),
        in_specs=[vmem, vmem],
        out_specs=(block, block),
        compiler_params=pltpu.CompilerParams(vmem_limit_bytes=GRANT),
        name="combine",
    )(lhs, table)


def shards(vectors, conduction, valence, hole_point, kpoint_grid, image_cells):
    points = conduction.shape[4]
    cond = conduction.reshape(4, 8, points)
    val = valence.reshape(32, points)
    lhs, table = run_exchange(
        RING,
        lax.axis_size("img"),
        NC,
        hole_point.reshape(1, 1),
        vectors,
        cond,
        val,
        kpoint_grid,
        image_cells,
    )
    real, imag = run_combine(lhs, table)
    shape = (16, 1, PTS, 512)
    return real.reshape(shape), imag.reshape(shape)


def solution(mesh):
    placed = (
        P(None, "img", "kgrp"),
        P("kgrp", None, None, "img", None),
        P("kgrp", None, None, "img", None),
        P(),
        P(),
        P(),
    )
    return jax.shard_map(
        shards,
        mesh=mesh,
        in_specs=placed,
        out_specs=(P(None, "img", "kgrp", None), P(None, "img", "kgrp", None)),
        check_vma=False,
    )
```

```python
import contextlib
import functools

import jax
import jax.numpy as jnp
import numpy as np
from jax import lax
from jax.experimental import pallas as pl
from jax.experimental.pallas import tpu as pltpu
from jax.sharding import PartitionSpec as P

MESH = pl.DeviceIdType.MESH
RING = (8, 4, 4)
NV = 8
NC = 8
LANES = 128
PTS = 32
GRANT = 24 * 1024 * 1024


def stage(name):
    return contextlib.nullcontext()


def drain(sem, ref):
    pltpu.make_async_copy(ref, ref, sem).wait()


COS30 = float(np.float32(jnp.bfloat16(np.cos(np.pi / 6))))
FIT = np.linalg.solve(
    np.array([[1.0, 1.0, 1.0], [1.0, 4.0, 16.0], [1.0, 9.0, 81.0]]),
    np.array([0.5, COS30 / 2, 1.0 / 3]),
)


def cosine(level):
    u = jnp.abs(level - 6.0) - 3.0
    square = u * u
    return u * (float(FIT[0]) + square * (float(FIT[1]) + square * float(FIT[2])))


def phases(kpt_ref, cell_ref, table):
    bf16, f32 = jnp.bfloat16, jnp.float32
    kpt = kpt_ref[...].astype(f32)
    cell = cell_ref[...].astype(f32)
    kpt = jnp.concatenate([kpt, jnp.zeros((5, kpt.shape[1]), f32)], 0).astype(bf16)
    cell = jnp.concatenate([cell, jnp.zeros((5, cell.shape[1]), f32)], 0).astype(bf16)
    rows = lax.broadcasted_iota(jnp.int32, (256, 256), 0)
    columns = lax.broadcasted_iota(jnp.int32, (256, 256), 1)
    source = 2 * jnp.bitwise_and(columns, 127) + jnp.right_shift(columns, 7)
    swap = jnp.where(rows == source, 1.0, 0.0).astype(bf16)
    kpt = jnp.dot(kpt, swap, preferred_element_type=f32)
    for a in range(2):
        part = jnp.transpose(kpt[:, a * 128 : a * 128 + 128]).astype(bf16)
        turns = jnp.dot(part, cell, preferred_element_type=f32)
        turns = turns - 12.0 * jnp.floor((turns + 0.5) * (1.0 / 12.0))
        cos = cosine(turns).astype(bf16)
        shifted = turns - 3.0
        sin = cosine(jnp.where(shifted < 0.0, shifted + 12.0, shifted)).astype(bf16)
        table[a * 256 : a * 256 + 128, 0:512] = cos
        table[a * 256 : a * 256 + 128, 512:1024] = sin
        table[a * 256 + 128 : a * 256 + 256, 0:512] = -sin
        table[a * 256 + 128 : a * 256 + 256, 512:1024] = cos


def exchange(
    ring,
    groups,
    nc,
    hole_hbm,
    vec_hbm,
    cond_hbm,
    val_hbm,
    kpt_hbm,
    cell_hbm,
    lhs,
    table,
    hole_v,
    vec_v,
    kpt_v,
    cell_v,
    cond_v,
    val_v,
    dest,
    cx,
    cy,
    cf,
    cs,
    ct,
    vf,
    hx,
    hz,
    hq,
    hw,
    hs,
    wf,
    wt,
    load_sem,
    cx_send,
    cx_recv,
    cy_send,
    cy_recv,
    cz_send,
    cz_recv,
    vy_send,
    vy_recv,
    vz_send,
    vz_recv,
    vx_send,
    vx_recv,
    hy_send,
    hy_recv,
    hz_send,
    hz_recv,
    hx_send,
    hx_recv,
    w_send,
    w_recv,
):
    ny, nx, nz = ring
    count = ny * nx * nz
    me = lax.axis_index("kgrp")
    img = lax.axis_index("img")
    y = lax.div(me, nx * nz)
    x = lax.rem(lax.div(me, nz), nx)
    z = lax.rem(me, nz)
    bf16, f32 = jnp.bfloat16, jnp.float32

    def at(yy, xx, zz, gg):
        return ((yy * nx + xx) * nz + zz, gg)

    def y_peer(step):
        yy = lax.rem(y + step, ny)
        return yy, at(yy, x, z, img)

    def x_peer(step):
        xx = lax.rem(x + step, nx)
        return xx, at(y, xx, z, img)

    def z_peer(step):
        zz = lax.rem(z + step, nz)
        return zz, at(y, x, zz, img)

    def img_peer(step):
        return (me, jnp.bitwise_xor(img, step))

    def corner(step, flip):
        return at(y, lax.rem(x + step, nx), z, jnp.bitwise_xor(img, flip))

    def send(src, dst, send_sem, recv_sem, device):
        pltpu.make_async_remote_copy(
            src_ref=src,
            dst_ref=dst,
            send_sem=send_sem,
            recv_sem=recv_sem,
            device_id=device,
            device_id_type=MESH,
        ).start()

    far_y = sorted(range(1, ny), key=lambda s: -min(s, ny - s))
    far_z = sorted(range(1, nz), key=lambda s: -min(s, nz - s))
    far_x = sorted(range(1, nx), key=lambda s: -min(s, nx - s))
    far_g = list(range(groups - 1, 0, -1))
    order = far_z + [0]

    barrier = pltpu.get_barrier_semaphore()
    peers = (
        [y_peer(s)[1] for s in far_y]
        + [z_peer(s)[1] for s in far_z]
        + [x_peer(s)[1] for s in far_x]
        + [img_peer(s) for s in far_g]
        + [corner(s, t) for s in far_x for t in far_g]
    )
    with stage("signal"):
        for peer in peers:
            pl.semaphore_signal(barrier, inc=1, device_id=peer, device_id_type=MESH)
    load_vec = pltpu.make_async_copy(vec_hbm, vec_v, load_sem.at[2])
    load_hole = pltpu.make_async_copy(hole_hbm, hole_v, load_sem.at[3])
    load_val = pltpu.make_async_copy(val_hbm, val_v, load_sem.at[0])
    load_cond = pltpu.make_async_copy(cond_hbm, cond_v, load_sem.at[1])
    load_kpt = pltpu.make_async_copy(kpt_hbm, kpt_v, load_sem.at[4])
    load_cell = pltpu.make_async_copy(cell_hbm, cell_v, load_sem.at[5])
    for load in (load_vec, load_hole, load_val, load_cond, load_kpt, load_cell):
        load.start()

    with stage("pack"):
        load_vec.wait()
        vf[y, x, z] = vec_v[...].reshape(8, vec_v.shape[2]).astype(vf.dtype)

    with stage("pick"):
        points = val_v.shape[1]
        load_hole.wait()
        wanted = hole_v[...] - img * points
        lane8 = lax.broadcasted_iota(jnp.int32, (8, LANES), 1)
        lane32 = lax.broadcasted_iota(jnp.int32, (32, LANES), 1)
        load_val.wait()

        def pick(j, kept):
            tile = val_v[:, pl.ds(pl.multiple_of(j * LANES, LANES), LANES)]
            return kept + jnp.where(lane32 + j * LANES == wanted, tile.astype(f32), 0.0)

        tile = lax.fori_loop(
            0, points // LANES, pick, jnp.zeros((32, LANES), f32), unroll=8
        )
        tile = jnp.concatenate([tile, jnp.zeros((LANES - 32, LANES), f32)], 0)
        tile = pltpu.roll(tile, z * 32, 0).astype(bf16)
        chosen = jnp.ones((8, LANES), bf16)
        row = lax.dot_general(
            chosen, tile, (((1,), (1,)), ((), ())), preferred_element_type=f32
        )
        hx[x, img] = row[0:1]

    low = lane8 < 64
    odd = lax.rem(lax.div(lane8, 32), 2) == 1

    def relay(j, carry):
        yy = lax.div(j, nx)
        xx = lax.rem(j, nx)
        column = pl.ds(pl.multiple_of(j * LANES, LANES), LANES)
        t = [cond_v[q, :, column].astype(f32) for q in range(4)]
        halves = []
        for q in range(2):
            halves.append(jnp.where(low, t[q], pltpu.roll(t[q + 2], 64, 1)))
        for q in range(2):
            halves.append(jnp.where(low, pltpu.roll(t[q], 64, 1), t[q + 2]))
        for h in range(2):
            first, second = halves[2 * h], halves[2 * h + 1]
            dest[yy, xx, 2 * h] = jnp.where(odd, pltpu.roll(second, 32, 1), first).astype(bf16)
            dest[yy, xx, 2 * h + 1] = jnp.where(odd, second, pltpu.roll(first, 96, 1)).astype(bf16)
        return carry

    with stage("relay"):
        load_cond.wait()
        lax.fori_loop(0, ny * nx, relay, 0, unroll=16)
        for zz in range(nz):
            for yy in range(ny):
                cx[zz, x, yy] = dest[yy, x, zz]

    with stage("barrier"):
        pl.semaphore_wait(barrier, len(peers))

    mine = hx.at[x, img]
    for s in far_x:
        for t in far_g:
            send(mine, mine, hx_send, hx_recv, corner(s, t))
        send(mine, mine, hx_send, hx_recv, x_peer(s)[1])
    for t in far_g:
        send(mine, mine, hx_send, hx_recv, img_peer(t))
    for s in far_y:
        send(vf.at[y, x, z], vf.at[y, x, z], vy_send, vy_recv, y_peer(s)[1])
    for s in order:
        zz = lax.rem(z + s, nz)
        for t in far_x:
            xx, device = x_peer(t)
            send(dest.at[:, xx, zz], cx.at[zz, x], cx_send, cx_recv.at[s], device)

    with stage("phases"):
        load_kpt.wait()
        load_cell.wait()
        if count == LANES:
            phases(kpt_v, cell_v, table)

    def wait_x(s):
        zz = lax.rem(z + s, nz)
        with stage(f"cx{s}"):
            drain(cx_recv.at[s], cx.at[zz, pl.ds(0, nx - 1)])

    def forward_y(s):
        zz = lax.rem(z + s, nz)
        for t in far_y:
            yy, device = y_peer(t)
            send(cx.at[zz, :, yy], cy.at[zz, y], cy_send, cy_recv.at[s], device)
        for xx in range(nx):
            cy[zz, y, xx] = cx[zz, xx, y]

    def wait_holes(sem):
        pltpu.make_async_copy(hw, hw, sem).wait()

    with stage("hole_x"):
        wait_holes(hx_recv)
        for xx in range(nx):
            total = hx[xx, 0]
            for t in range(1, groups):
                total = total + hx[xx, t]
            hz[z, xx] = total
    wait_x(order[0])
    forward_y(order[0])
    for t in far_z:
        send(hz.at[z], hz.at[z], hz_send, hz_recv, z_peer(t)[1])
    wait_x(order[1])
    forward_y(order[1])

    with stage("vec_y"):
        drain(vy_recv, vf.at[pl.ds(0, ny - 1), 0, 0])
    for t in far_z:
        send(vf.at[:, x, z], vf.at[:, x, z], vz_send, vz_recv.at[t], z_peer(t)[1])
    for t in far_x:
        send(vf.at[:, x, z], vf.at[:, x, z], vx_send, vx_recv, x_peer(t)[1])
    for s in order[2:]:
        wait_x(s)
        forward_y(s)

    def forward_v(t):
        zz = lax.rem(z + nz - t, nz)
        with stage(f"vec_z{t}"):
            drain(vz_recv.at[t], vf.at[:, 0, 0])
        for u in far_x:
            send(vf.at[:, x, zz], vf.at[:, x, zz], vx_send, vx_recv, x_peer(u)[1])

    def forward_z(s):
        zz, device = z_peer(s)
        with stage(f"cy{s}"):
            drain(cy_recv.at[s], cy.at[zz, pl.ds(0, ny - 1)])
        send(cy.at[zz], cf.at[:, :, z], cz_send, cz_recv, device)

    near_z = far_z[::-1]
    with stage("hole_z"):
        drain(hz_recv, hz.at[pl.ds(0, nz - 1)])
        packed = hz[0]
        for t in range(1, nz):
            packed = packed + hz[t]
        hq[y] = packed
    for t in near_z[:-1]:
        forward_v(t)
    for s in far_y:
        send(hq.at[y], hq.at[y], hy_send, hy_recv, y_peer(s)[1])
    forward_z(far_z[0])
    forward_v(near_z[-1])
    for s in far_z[1:]:
        forward_z(s)

    with stage("cy0"):
        drain(cy_recv.at[0], cy.at[z, pl.ds(0, ny - 1)])
        for yy in range(ny):
            for xx in range(nx):
                cf[yy, xx, z] = cy[z, yy, xx]

    with stage("vec_x"):
        drain(vx_recv, vf.at[:, pl.ds(0, nx - 1)])
    with stage("hole_y"):
        drain(hy_recv, hq.at[pl.ds(0, ny - 1)])

    with stage("weights"):
        part = hq[...].reshape(ny * nx, LANES)
        for zz in range(nz):
            turned = part if zz == 0 else pltpu.roll(part, LANES - 32 * zz, 1)
            hs[pl.ds(zz, ny * nx, nz), :] = turned
        holes = jnp.transpose(hs[...])
        upper = lax.broadcasted_iota(jnp.int32, (8, vf.shape[4]), 0) < 4
        for a in range(2):
            for c in range(nc):
                along = None
                across = None
                for v in range(NV):
                    d = (a * NV + v) * nc + c
                    piece = vf[d // (nx * nz), d // nz % nx, d % nz].astype(f32)
                    real = piece * holes[a * 16 + v : a * 16 + v + 1]
                    imag = piece * holes[a * 16 + 8 + v : a * 16 + 9 + v]
                    along = real if along is None else along + real
                    across = imag if across is None else across + imag
                across = pltpu.roll(across, 4, 0)
                weight = (along + jnp.where(upper, across, -across)) * ((NV * NC) ** -0.5)
                wf[img, a * nc + c] = weight.astype(bf16)

    for s in far_g[::-1]:
        send(wf.at[img], wf.at[img], w_send, w_recv.at[s], img_peer(s))
    with stage("cz"):
        drain(cz_recv, cf.at[:, :, pl.ds(0, nz - 1)])
    with stage("turn"):
        cs[...] = cf[...].astype(f32).reshape(cs.shape)
        for c in range(8):
            ct[c] = jnp.transpose(cs[pl.ds(c, count, 8), :])

    def products(step):
        group = jnp.bitwise_xor(img, step)
        wt[...] = wf[group].astype(f32)
        for a in range(2):
            for half in range(2):
                reals = []
                imags = []
                for c in range(nc):
                    start = a * 64 + half * 16
                    reals.append(ct[c, start : start + 16, :])
                    imags.append(ct[c, start + 32 : start + 48, :])
                for s in range(4):
                    out_real = None
                    out_imag = None
                    for c in range(nc):
                        wr = wt[a * nc + c, s : s + 1, :]
                        wi = wt[a * nc + c, s + 4 : s + 5, :]
                        tr = wr * reals[c] - wi * imags[c]
                        ti = wr * imags[c] + wi * reals[c]
                        out_real = tr if out_real is None else out_real + tr
                        out_imag = ti if out_imag is None else out_imag + ti
                    first = pl.multiple_of(group * 128 + (s * 32 + half * 16), 16)
                    left = a * 2 * count
                    here = pl.ds(first, 16)
                    lhs[here, left : left + count] = out_real.astype(bf16)
                    lhs[here, left + count : left + 2 * count] = out_imag.astype(bf16)

    with stage("own"):
        products(0)
    for s in far_g[::-1]:
        with stage(f"wimg{s}"):
            drain(w_recv.at[s], wf.at[0])
        with stage("products"):
            products(s)

    with stage("sends"):
        drain(vy_send, vf.at[pl.ds(0, ny - 1), 0, 0])
        drain(vz_send, vf.at[:, 0, pl.ds(0, nz - 1)])
        drain(vx_send, vf.at[:, pl.ds(0, nx - 1)])
        drain(hy_send, hq.at[pl.ds(0, ny - 1)])
        drain(hz_send, hz.at[pl.ds(0, nz - 1)])
        wait_holes(hx_send)
        drain(cx_send, cx.at[:, pl.ds(0, nx - 1)])
        drain(cy_send, cy.at[:, pl.ds(0, ny - 1)])
        drain(cz_send, cf.at[:, :, pl.ds(0, nz - 1)])
        drain(w_send, wf.at[pl.ds(0, groups - 1)])


def run_exchange(ring, groups, nc, hole, vec, cond, val, kpt, cell, vec_type=jnp.bfloat16):
    ny, nx, nz = ring
    count = ny * nx * nz
    lanes = vec.shape[2]
    bf16, f32, i32 = jnp.bfloat16, jnp.float32, jnp.int32
    dma = pltpu.SemaphoreType.DMA
    rows = groups * 4 * PTS
    anywhere = pl.BlockSpec(memory_space=pltpu.HBM)
    vmem = pl.BlockSpec(memory_space=pltpu.VMEM)
    scratch = [
        pltpu.VMEM(hole.shape, i32),
        pltpu.VMEM(vec.shape, f32),
        pltpu.VMEM(kpt.shape, i32),
        pltpu.VMEM(cell.shape, i32),
        pltpu.VMEM(cond.shape, bf16),
        pltpu.VMEM(val.shape, bf16),
        pltpu.VMEM((ny, nx, nz, 8, LANES), bf16),
        pltpu.VMEM((nz, nx, ny, 8, LANES), bf16),
        pltpu.VMEM((nz, ny, nx, 8, LANES), bf16),
        pltpu.VMEM((ny, nx, nz, 8, LANES), bf16),
        pltpu.VMEM((count * 8, LANES), f32),
        pltpu.VMEM((8, LANES, count), f32),
        pltpu.VMEM((ny, nx, nz, 8, lanes), vec_type),
        pltpu.VMEM((nx, groups, 1, LANES), f32),
        pltpu.VMEM((nz, nx, 1, LANES), f32),
        pltpu.VMEM((ny, nx, 1, LANES), f32),
        pltpu.VMEM((nx * groups - 1, 1, LANES), f32),
        pltpu.VMEM((count, LANES), f32),
        pltpu.VMEM((groups, 2 * nc, 8, lanes), bf16),
        pltpu.VMEM((2 * nc, 8, lanes), f32),
        dma((6,)),
        dma(()),
        dma((nz,)),
        dma(()),
        dma((nz,)),
        dma(()),
        dma(()),
        dma(()),
        dma(()),
        dma(()),
        dma((nz,)),
        dma(()),
        dma(()),
        dma(()),
        dma(()),
        dma(()),
        dma(()),
        dma(()),
        dma(()),
        dma(()),
        dma((groups,)),
    ]
    return pl.pallas_call(
        functools.partial(exchange, ring, groups, nc),
        out_shape=(
            jax.ShapeDtypeStruct((rows, 4 * count), bf16),
            jax.ShapeDtypeStruct((512, 1024), bf16),
        ),
        in_specs=[anywhere] * 6,
        out_specs=(vmem, vmem),
        scratch_shapes=scratch,
        compiler_params=pltpu.CompilerParams(
            collective_id=0, has_side_effects=True, vmem_limit_bytes=GRANT
        ),
        name="exchange",
    )(hole, *(pltpu.with_memory_space_constraint(v, pltpu.HBM) for v in (vec, cond, val, kpt, cell)))


def combine(lhs, table, real_ref, imag_ref):
    half = real_ref.shape[1]
    scale = 512.0**-0.5
    for part, ref in ((0, real_ref), (1, imag_ref)):
        start = pl.multiple_of(part * 512 + pl.program_id(0) * half, half)
        ref[...] = (
            jnp.dot(lhs[...], table[:, pl.ds(start, half)], preferred_element_type=jnp.float32)
            * scale
        )


def run_combine(lhs, table):
    rows = lhs.shape[0]
    vmem = pl.BlockSpec(memory_space=pltpu.VMEM)
    block = pl.BlockSpec((rows, 256), lambda i: (0, i))
    return pl.pallas_call(
        combine,
        grid=(2,),
        out_shape=(
            jax.ShapeDtypeStruct((rows, 512), jnp.float32),
            jax.ShapeDtypeStruct((rows, 512), jnp.float32),
        ),
        in_specs=[vmem, vmem],
        out_specs=(block, block),
        compiler_params=pltpu.CompilerParams(vmem_limit_bytes=GRANT),
        name="combine",
    )(lhs, table)


def shards(vectors, conduction, valence, hole_point, kpoint_grid, image_cells):
    points = conduction.shape[4]
    cond = conduction.reshape(4, 8, points)
    val = valence.reshape(32, points)
    lhs, table = run_exchange(
        RING,
        lax.axis_size("img"),
        NC,
        hole_point.reshape(1, 1),
        vectors,
        cond,
        val,
        kpoint_grid,
        image_cells,
    )
    real, imag = run_combine(lhs, table)
    shape = (16, 1, PTS, 512)
    return real.reshape(shape), imag.reshape(shape)


def solution(mesh):
    placed = (
        P(None, "img", "kgrp"),
        P("kgrp", None, None, "img", None),
        P("kgrp", None, None, "img", None),
        P(),
        P(),
        P(),
    )
    return jax.shard_map(
        shards,
        mesh=mesh,
        in_specs=placed,
        out_specs=(P(None, "img", "kgrp", None), P(None, "img", "kgrp", None)),
        check_vma=False,
    )
```
